32 devices in a mesh: groups: 2 (over x), space: 16 (over z, y, core).
Axes of the slice: x: 2, y: 2, z: 4, core: 2. Of those that a mesh axis runs over, the one named last changes fastest.
Arguments:
- hidden: bfloat16 [4096, 512], P(('groups', 'space')), parts along dimension 0, may hold values from -130 to 130
- norm_gain: float32 [512], replicated, may hold values from 0.5 to 2
- norm_shift: float32 [512], replicated, may hold values from -3 to 3
- conv_weight: bfloat16 [3, 3, 3, 512, 512], P(None, None, None, 'space'), may hold values from -0.0546875 to 0.0546875
- conv_bias: bfloat16 [512], replicated, may hold values from -3 to 3
Outputs:
- decoded: bfloat16 [8, 32, 64, 512], P('groups', None, 'space'), parts along dimension 0
The draws below stay inside these ranges and needn't reach their ends.
There are 2 independent parts, one for each index of `groups`. The reference program is written for one: setup_inputs(seed, part) draws one part's arguments, and reference() takes and returns one part's arrays. A program takes and returns all parts, laid end to end along the dimension named above; an argument that names none is the same for every part. Nothing has to cross between parts.
All inputs are finite; a program needn't handle non-finite values.
Results may differ from the reference program's by a relative error of at most 0.0045.
Values may be sent and summed in bfloat16 or wider, within the bound.
A program may use at most 64 MiB of HBM per device.

```python
import math
import jax
import jax.numpy as jnp
from jax import lax

CHANNELS = 512
GROUPS = 32
FRAMES = 4
ROWS = 16
WIDTH = 32
TOKENS = 2048


def draw_hidden(key, part):
    keys = jax.random.split(jax.random.fold_in(key, 11), 3)
    column = (jnp.arange(TOKENS) % WIDTH).astype(jnp.float32)
    ramp = 1.0 + 2.0 * column / max(WIDTH - 1, 1)
    channel_scale = jnp.exp(jax.random.uniform(keys[1], (CHANNELS,), jnp.float32, 0.0, math.log(10.0)))
    channel_mean = jnp.clip(0.5 * jax.random.normal(keys[2], (CHANNELS,), jnp.float32), -1.5, 1.5)
    base = jnp.clip(jax.random.normal(keys[0], (TOKENS, CHANNELS), jnp.float32), -4.0, 4.0)
    return (base * ramp[:, None] * channel_scale[None, :] + channel_mean[None, :]).astype(jnp.bfloat16)


def level_of(own_key, dims, shards, smallest, high):
    factor_of, own = 1.0, jax.random.fold_in(own_key, 6)
    for axis_at, blocks in shards:
        steps = jnp.exp(jax.random.uniform(jax.random.fold_in(own, axis_at), (blocks,), jnp.float32, smallest / len(shards), high / len(shards)))
        factor_of = factor_of * jnp.repeat(steps, dims[axis_at] // blocks).reshape([-1 if axis == axis_at else 1 for axis in range(len(dims))])
    return factor_of


def bell_draw(own_key, shape, scale, bound, shards=(), dtype=jnp.bfloat16):
    values = scale * jax.random.normal(own_key, shape, jnp.float32)
    if shards:
        values = values * level_of(own_key, shape, shards, -0.22, 0.18)
    return jnp.clip(values, -bound, bound).astype(dtype)


def setup_inputs(seed: int = 0, part: int = 0) -> dict:
    streams_of = jax.random.split(jax.random.key(seed), 6)
    part_keys = jax.random.split(jax.random.fold_in(streams_of[5], part), 6)
    return {
        "hidden": draw_hidden(jax.random.fold_in(jax.random.fold_in(streams_of[5], part), 71), part),
        "norm_gain": jnp.clip(jnp.exp(jax.random.uniform(streams_of[1], (CHANNELS,), jnp.float32, math.log(0.5), math.log(2.0))), 0.5, 2.0),
        "norm_shift": bell_draw(streams_of[2], (CHANNELS,), 0.5, 3.0, (), jnp.float32),
        "conv_weight": bell_draw(streams_of[3], (3, 3, 3, CHANNELS, CHANNELS), (27 * CHANNELS) ** -0.5, 0.0546875, ((3, 16),)),
        "conv_bias": bell_draw(streams_of[4], (CHANNELS,), 0.5, 3.0),
    }


EPSILON = 1e-06

def reference(hidden, norm_gain, norm_shift, conv_weight, conv_bias):
    values = hidden.astype(jnp.float32).reshape(FRAMES, ROWS, WIDTH, GROUPS, CHANNELS // GROUPS)
    average = lax.optimization_barrier(jnp.mean(values, axis=(0, 1, 2, 4), keepdims=True))
    spread = lax.optimization_barrier(jnp.mean((values - average) ** 2, axis=(0, 1, 2, 4), keepdims=True))
    normed = ((values - average) * lax.rsqrt(spread + EPSILON)).reshape(FRAMES, ROWS, WIDTH, CHANNELS)
    active = jax.nn.silu(normed * norm_gain + norm_shift).astype(jnp.bfloat16)
    doubled = jnp.repeat(jnp.repeat(active, 2, axis=1), 2, axis=2)
    padded = jnp.pad(doubled, ((2, 0), (1, 1), (1, 1), (0, 0)), mode='edge')
    result = lax.conv_general_dilated(padded[None].astype(jnp.float32), conv_weight.astype(jnp.float32), (1, 1, 1), 'VALID', dimension_numbers=('NDHWC', 'DHWIO', 'NDHWC'))[0]
    return (result + conv_bias.astype(jnp.float32)).astype(jnp.bfloat16)
```

```python
import jax
import jax.numpy as jnp
from jax import lax
from jax.sharding import PartitionSpec as P

GROUPS = 32
FRAMES = 4
ROWS = 16
EPSILON = 1e-06


def normalised(hidden, gain, shift):
    cells, channels = hidden.shape
    values = hidden.astype(jnp.float32)
    member = (
        jnp.arange(channels)[:, None] // (channels // GROUPS)
        == jnp.arange(channels)[None, :] // (channels // GROUPS)
    ).astype(jnp.float32)
    population = float(cells * (channels // GROUPS))

    def spread_out(v):
        return jnp.dot(v[None], member, precision=lax.Precision.HIGHEST)[0] / population

    average = spread_out(jnp.sum(values, axis=0))
    spread = spread_out(jnp.sum((values - average) ** 2, axis=0))
    scale = lax.rsqrt(spread + EPSILON) * gain
    return jax.nn.silu((values - average) * scale + shift).astype(jnp.bfloat16)


def clamp_shift(x, axis, step):
    length = x.shape[axis]
    if step < 0:
        return jnp.concatenate(
            [lax.slice_in_dim(x, 0, 1, axis=axis), lax.slice_in_dim(x, 0, length - 1, axis=axis)],
            axis=axis,
        )
    return jnp.concatenate(
        [lax.slice_in_dim(x, 1, length, axis=axis), lax.slice_in_dim(x, length - 1, length, axis=axis)],
        axis=axis,
    )


def phases(first, middle, last, axis):
    early = clamp_shift(first, axis, -1) + (middle + last)
    late = (first + middle) + clamp_shift(last, axis, 1)
    return early, late


def shards(hidden, norm_gain, norm_shift, conv_weight, conv_bias):
    devices = lax.axis_size("space")
    channels = hidden.shape[1]
    own = channels // devices
    mine = lax.all_to_all(conv_weight, "space", split_axis=4, concat_axis=3, tiled=True)
    cells = lax.all_gather(hidden, "space", axis=0, tiled=True)
    width = cells.shape[0] // (FRAMES * ROWS)
    active = normalised(cells, norm_gain, norm_shift).reshape(FRAMES, ROWS, width, channels)
    first = active[:1]
    history = jnp.concatenate([first, first, active], axis=0)
    kernel = jnp.transpose(mine, (0, 3, 1, 2, 4)).reshape(3, channels, 9 * own)
    taps = sum(
        lax.dot_general(
            history[a : a + FRAMES].reshape(-1, channels),
            kernel[a],
            (((1,), (0,)), ((), ())),
            preferred_element_type=jnp.float32,
        )
        for a in range(3)
    ).reshape(FRAMES, ROWS, width, 3, 3, own)
    rows = phases(taps[..., 0, :, :], taps[..., 1, :, :], taps[..., 2, :, :], 1)
    cols = [phases(r[..., 0, :], r[..., 1, :], r[..., 2, :], 2) for r in rows]
    result = jnp.stack([jnp.stack(c, axis=3) for c in cols], axis=2)
    result = result.reshape(FRAMES, 2 * ROWS, 2 * width, own)
    bias = lax.dynamic_slice_in_dim(conv_bias, lax.axis_index("space") * own, own)
    decoded = (result + bias.astype(jnp.float32)).astype(jnp.bfloat16)
    return lax.all_to_all(decoded, "space", split_axis=2, concat_axis=3, tiled=True)


def solution(mesh):
    placed = (P(("groups", "space"), None), P(), P(), P(None, None, None, "space", None), P())
    return jax.shard_map(
        shards,
        mesh=mesh,
        in_specs=placed,
        out_specs=P("groups", None, "space", None),
        check_vma=False,
    )
```

```python
import functools

import jax
import jax.numpy as jnp
from jax import lax
from jax.experimental import pallas as pl
from jax.experimental.pallas import tpu as pltpu
from jax.sharding import PartitionSpec as P

GROUPS = 32
FRAMES = 4
ROWS = 16
EPSILON = 1e-06
LANES = 128
MESH = pl.DeviceIdType.MESH


def normalised(hidden, gain, shift):
    cells, channels = hidden.shape
    values = hidden.astype(jnp.float32)
    member = (
        jnp.arange(channels)[:, None] // (channels // GROUPS)
        == jnp.arange(channels)[None, :] // (channels // GROUPS)
    ).astype(jnp.float32)
    population = float(cells * (channels // GROUPS))

    def spread_out(v):
        return jnp.dot(v[None], member, precision=lax.Precision.HIGHEST)[0] / population

    average = spread_out(jnp.sum(values, axis=0))
    spread = spread_out(jnp.sum((values - average) ** 2, axis=0))
    scale = lax.rsqrt(spread + EPSILON) * gain
    return jax.nn.silu((values - average) * scale + shift).astype(jnp.bfloat16)


def clamp_shift(x, axis, step):
    length = x.shape[axis]
    if step < 0:
        return jnp.concatenate(
            [lax.slice_in_dim(x, 0, 1, axis=axis), lax.slice_in_dim(x, 0, length - 1, axis=axis)],
            axis=axis,
        )
    return jnp.concatenate(
        [lax.slice_in_dim(x, 1, length, axis=axis), lax.slice_in_dim(x, length - 1, length, axis=axis)],
        axis=axis,
    )


def phases(first, middle, last, axis):
    early = clamp_shift(first, axis, -1) + (middle + last)
    late = (first + middle) + clamp_shift(last, axis, 1)
    return early, late


def shards(hidden, norm_gain, norm_shift, conv_weight, conv_bias):
    devices = lax.axis_size("space")
    channels = hidden.shape[1]
    own = channels // devices
    mine = lax.all_to_all(conv_weight, "space", split_axis=4, concat_axis=3, tiled=True)
    cells = lax.all_gather(hidden, "space", axis=0, tiled=True)
    width = cells.shape[0] // (FRAMES * ROWS)
    active = normalised(cells, norm_gain, norm_shift).reshape(FRAMES, ROWS, width, channels)
    first = active[:1]
    history = jnp.concatenate([first, first, active], axis=0)
    kernel = jnp.transpose(mine, (0, 3, 1, 2, 4)).reshape(3, channels, 9 * own)
    taps = sum(
        lax.dot_general(
            history[a : a + FRAMES].reshape(-1, channels),
            kernel[a],
            (((1,), (0,)), ((), ())),
            preferred_element_type=jnp.float32,
        )
        for a in range(3)
    ).reshape(FRAMES, ROWS, width, 3, 3, own)
    rows = phases(taps[..., 0, :, :], taps[..., 1, :, :], taps[..., 2, :, :], 1)
    cols = [phases(r[..., 0, :], r[..., 1, :], r[..., 2, :], 2) for r in rows]
    result = jnp.stack([jnp.stack(c, axis=3) for c in cols], axis=2)
    result = result.reshape(FRAMES, 2 * ROWS, 2 * width, own)
    bias = lax.dynamic_slice_in_dim(conv_bias, lax.axis_index("space") * own, own)
    decoded = (result + bias.astype(jnp.float32)).astype(jnp.bfloat16)
    return lax.all_to_all(decoded, "space", split_axis=2, concat_axis=3, tiled=True)


def fused(dims, hid_ref, gain_ref, shift_ref, w_ref, bias_ref, out_ref, acts, active, packed, weights,
          total, leaving, arrived, final, act_send, act_recv, sis_send, w_send, w_recv, x_send, o_send, o_recv):
    parts, n, own, tokens, channels, width = dims
    chips = n // 2
    g, s = lax.axis_index("groups"), lax.axis_index("space")
    chip, core = s // 2, s % 2
    odd = chip % 2
    place = (1 - odd) * (chip // 2) + odd * (chips - 1 - chip // 2)

    def device_at(p):
        p = lax.rem(p + 2 * chips, chips)
        far = p // (chips // 2)
        return ((1 - far) * 2 * p + far * (2 * (chips - 1 - p) + 1)) * 2 + core

    right, left = device_at(place + 1), device_at(place - 1)
    sister = chip * 2 + 1 - core
    sends = s % parts == g

    def remote(source, target, send, recv, device, group=None):
        return pltpu.make_async_remote_copy(
            src_ref=source, dst_ref=target, send_sem=send, recv_sem=recv,
            device_id=(g if group is None else group, device), device_id_type=MESH,
        )

    barrier = pltpu.get_barrier_semaphore()
    for k in range(1, n):
        pl.semaphore_signal(barrier, inc=1, device_id=(g, lax.rem(s + k, n)), device_id_type=MESH)
    for k in range(1, parts):
        pl.semaphore_signal(barrier, inc=1, device_id=(lax.rem(g + k, parts), s), device_id_type=MESH)

    @pl.when(sends)
    def _():
        @pl.loop(0, 9)
        def _(ab):
            rows = [w_ref[3 * ab + e] for e in range(3)]
            for d in range(n):
                lanes = [r[:, d * own : (d + 1) * own] for r in rows]
                block = jnp.concatenate(lanes + [jnp.zeros_like(lanes[0])], axis=1)
                packed[d, ab] = block

    acts[s] = hid_ref[...]
    pl.semaphore_wait(barrier, n - 1 + parts - 1)

    pending = []

    def go(copy):
        copy.start()
        pending.append(copy)

    to_right, to_left = chips // 2, chips - 1 - chips // 2
    go(remote(hid_ref, acts.at[s], act_send.at[0, 0], act_recv.at[s], right))
    go(remote(hid_ref, acts.at[s], act_send.at[1, 0], act_recv.at[s], left))
    go(remote(hid_ref, acts.at[s], sis_send.at[0], act_recv.at[s], sister))

    outgoing = []
    for k in range(1, n):
        d = lax.rem(s + k, n)
        outgoing.append(remote(packed.at[d], weights.at[s], w_send.at[k], w_recv.at[s], d))

    @pl.when(sends)
    def _():
        for copy in outgoing:
            copy.start()
        weights[s] = packed[s]

    rounds = n // parts

    def relay(i):
        source = lax.rem(s // parts + i, rounds) * parts + g
        incoming = remote(weights.at[source], weights.at[source], x_send.at[i, 0], w_recv.at[source], s)
        if i == 0:
            @pl.when(s % parts != g)
            def _():
                incoming.wait_recv()
        else:
            incoming.wait_recv()
        for k in range(1, parts):
            go(remote(weights.at[source], weights.at[source], x_send.at[i, k], w_recv.at[source], s,
                      lax.rem(g + k, parts)))

    def arrival(source):
        remote(acts.at[source], acts.at[source], act_send.at[0, 0], act_recv.at[source], sister).wait_recv()

    relayed = 0
    for k in range(1, to_right + 1):
        for side, hops, step, onward in ((0, to_right, -k, right), (1, to_left, k, left)):
            if k > hops:
                continue
            source = device_at(place + step)
            arrival(source)
            if k < hops:
                go(remote(acts.at[source], acts.at[source], act_send.at[side, k], act_recv.at[source], onward))
            go(remote(acts.at[source], acts.at[source], sis_send.at[2 * k - 1 + side], act_recv.at[source], sister))
        while relayed < rounds * k // (to_right + 1):
            relay(relayed)
            relayed += 1
    for k in range(chips):
        arrival(k * 2 + 1 - core)

    size = channels // GROUPS
    population = float(n * tokens * size)
    lane = lax.broadcasted_iota(jnp.int32, (8, channels), 1)

    def over_group(v):
        v = jnp.broadcast_to(jnp.sum(v, axis=0, keepdims=True), (8, channels))
        step = 1
        while step < size:
            v = v + jnp.where(lane // step % 2 == 1, pltpu.roll(v, step, 1), pltpu.roll(v, channels - step, 1))
            step *= 2
        return v[:1] / population

    def add_rows(term):
        def body(i, carry):
            v = term(acts[i].astype(jnp.float32))
            return carry + jnp.sum(v.reshape(tokens // 8, 8, channels), axis=0)
        return lax.fori_loop(0, n, body, jnp.zeros((8, channels), jnp.float32))

    average = over_group(add_rows(lambda v: v))
    spread = over_group(add_rows(lambda v: (v - average) * (v - average)))
    scale = lax.rsqrt(spread + EPSILON) * gain_ref[...]
    offset = shift_ref[...]

    @pl.loop(0, n)
    def _(i):
        v = (acts[i].astype(jnp.float32) - average) * scale + offset
        active[i] = (v / (1.0 + jnp.exp(-v))).astype(jnp.bfloat16)

    while relayed < rounds:
        relay(relayed)
        relayed += 1
    for i in range(rounds):
        for k in range(1, parts):
            source = i * parts + lax.rem(g + k, parts)
            remote(weights.at[source], weights.at[source], x_send.at[i, 0], w_recv.at[source], s).wait_recv()

    per = n // FRAMES
    cells = ROWS * width
    column = lax.broadcasted_iota(jnp.int32, (cells, LANES), 0) % width
    lanes = lax.broadcasted_iota(jnp.int32, (cells, LANES), 1)
    bias = bias_ref[...]

    @pl.loop(0, FRAMES)
    def _(f):
        taps = jnp.zeros((cells, 3 * LANES), jnp.float32)
        for a in range(3):
            frame = jnp.maximum(f + (a - 2), 0)
            left_side = active[pl.ds(frame * per, per)].reshape(cells, channels)
            right_side = jnp.concatenate(
                [weights[:, 3 * a + b].reshape(channels, LANES) for b in range(3)], axis=1
            )
            taps = taps + jnp.dot(left_side, right_side, preferred_element_type=jnp.float32)
        first, middle, last = (taps[:, b * LANES : (b + 1) * LANES] for b in range(3))
        above = jnp.concatenate([first[:width], first[:-width]], axis=0)
        below = jnp.concatenate([last[width:], last[-width:]], axis=0)
        both = []
        for r in (above + (middle + last), (first + middle) + below):
            near = pltpu.roll(r, LANES - own, 1)
            far = pltpu.roll(r, LANES - 2 * own, 1)
            back = pltpu.roll(r, own, 1)
            before = jnp.where(column == 0, r, pltpu.roll(r, 1, 0))
            after = jnp.where(column == width - 1, near, pltpu.roll(near, cells - 1, 0))
            both.append(jnp.where(lanes < own, before + near + far, back + r + after))
        joined = jnp.where(lanes < 2 * own, both[0], pltpu.roll(both[1], 2 * own, 1))
        total[pl.ds(f * cells, cells)] = joined + bias

    local = width // n
    for d in range(n):
        for j in range(local):
            rows = total[pl.ds(d * local + j, FRAMES * ROWS, stride=width), :]
            leaving[d, j] = rows.astype(jnp.bfloat16)
    for k in range(1, n):
        d = lax.rem(s + k, n)
        go(remote(leaving.at[d], arrived.at[s], o_send.at[k], o_recv.at[s], d))
    arrived[s] = leaving[s]
    for k in range(1, n):
        source = lax.rem(s + n - k, n)
        remote(arrived.at[source], arrived.at[source], o_send.at[0], o_recv.at[source], s).wait_recv()

    quarter = lax.broadcasted_iota(jnp.int32, (FRAMES * ROWS, LANES), 1) // own
    for q in range(n // 4):
        for j in range(local):
            pieces = [arrived[4 * q + i, j].astype(jnp.float32) for i in range(4)]
            for phase in range(4):
                whole = pieces[phase]
                for i in range(4):
                    turned = pieces[i] if i == phase else pltpu.roll(pieces[i], (i - phase) % 4 * own, 1)
                    whole = turned if i == 0 else jnp.where(quarter == i, turned, whole)
                pr, pc = phase // 2, phase % 2
                at = (pr * local + j) * 2 + pc
                final[q, pl.ds(at, FRAMES * ROWS, stride=4 * local), :] = whole
    for q in range(n // 4):
        out_ref[:, q * LANES : (q + 1) * LANES] = final[q].astype(jnp.bfloat16)

    for copy in pending:
        copy.wait_send()

    @pl.when(sends)
    def _():
        for copy in outgoing:
            copy.wait_send()


def fused_shards(hidden, norm_gain, norm_shift, conv_weight, conv_bias):
    n, parts = lax.axis_size("space"), lax.axis_size("groups")
    tokens, channels = hidden.shape
    own = channels // n
    width = n * tokens // (FRAMES * ROWS)
    local = width // n
    bias = lax.dynamic_slice_in_dim(conv_bias, lax.axis_index("space") * own, own)
    bias = jnp.tile(bias.astype(jnp.float32), 4)[None]
    rows = FRAMES * 2 * ROWS * 2 * local
    bf16, f32 = jnp.bfloat16, jnp.float32
    dma = pltpu.SemaphoreType.DMA
    rounds = n // parts
    out = pl.pallas_call(
        functools.partial(fused, (parts, n, own, tokens, channels, width)),
        out_shape=jax.ShapeDtypeStruct((rows, channels), bf16),
        in_specs=[pl.BlockSpec(memory_space=pltpu.VMEM)] * 5,
        out_specs=pl.BlockSpec(memory_space=pltpu.VMEM),
        scratch_shapes=[
            pltpu.VMEM((n, tokens, channels), bf16),
            pltpu.VMEM((n, tokens, channels), bf16),
            pltpu.VMEM((n, 9, own, LANES), bf16),
            pltpu.VMEM((n, 9, own, LANES), bf16),
            pltpu.VMEM((n * tokens, LANES), f32),
            pltpu.VMEM((n, local, FRAMES * ROWS, LANES), bf16),
            pltpu.VMEM((n, local, FRAMES * ROWS, LANES), bf16),
            pltpu.VMEM((n // 4, rows, LANES), f32),
            dma((2, n // 4 + 1)),
            dma((n,)),
            dma((n,)),
            dma((n,)),
            dma((n,)),
            dma((rounds, parts)),
            dma((n,)),
            dma((n,)),
        ],
        compiler_params=pltpu.CompilerParams(
            collective_id=0, has_side_effects=True, vmem_limit_bytes=60 * 1024 * 1024
        ),
    )(
        hidden,
        norm_gain[None],
        norm_shift[None],
        conv_weight.reshape(27, own, channels),
        bias,
    )
    return out.reshape(FRAMES, 2 * ROWS, 2 * local, channels)


def pick(hidden, norm_gain, norm_shift, conv_weight, conv_bias):
    n, parts = lax.axis_size("space"), lax.axis_size("groups")
    own = hidden.shape[1] // n
    suits = own * 4 == LANES and n % 4 == 0 and n % parts == 0 and hidden.shape[0] % 16 == 0
    body = fused_shards if suits else shards
    return body(hidden, norm_gain, norm_shift, conv_weight, conv_bias)


def solution(mesh):
    placed = (P(("groups", "space"), None), P(), P(), P(None, None, None, "space", None), P())
    return jax.shard_map(
        pick,
        mesh=mesh,
        in_specs=placed,
        out_specs=P("groups", None, "space", None),
        check_vma=False,
    )
```

```python
import functools

import jax
import jax.numpy as jnp
from jax import lax
from jax.experimental import pallas as pl
from jax.experimental.pallas import tpu as pltpu
from jax.sharding import PartitionSpec as P

GROUPS = 32
FRAMES = 4
ROWS = 16
EPSILON = 1e-06
LANES = 128
PIECES = 2
MESH = pl.DeviceIdType.MESH


def normalised(hidden, gain, shift):
    cells, channels = hidden.shape
    values = hidden.astype(jnp.float32)
    member = (
        jnp.arange(channels)[:, None] // (channels // GROUPS)
        == jnp.arange(channels)[None, :] // (channels // GROUPS)
    ).astype(jnp.float32)
    population = float(cells * (channels // GROUPS))

    def spread_out(v):
        return jnp.dot(v[None], member, precision=lax.Precision.HIGHEST)[0] / population

    average = spread_out(jnp.sum(values, axis=0))
    spread = spread_out(jnp.sum((values - average) ** 2, axis=0))
    scale = lax.rsqrt(spread + EPSILON) * gain
    return jax.nn.silu((values - average) * scale + shift).astype(jnp.bfloat16)


def clamp_shift(x, axis, step):
    length = x.shape[axis]
    if step < 0:
        return jnp.concatenate(
            [lax.slice_in_dim(x, 0, 1, axis=axis), lax.slice_in_dim(x, 0, length - 1, axis=axis)],
            axis=axis,
        )
    return jnp.concatenate(
        [lax.slice_in_dim(x, 1, length, axis=axis), lax.slice_in_dim(x, length - 1, length, axis=axis)],
        axis=axis,
    )


def phases(first, middle, last, axis):
    early = clamp_shift(first, axis, -1) + (middle + last)
    late = (first + middle) + clamp_shift(last, axis, 1)
    return early, late


def shards(hidden, norm_gain, norm_shift, conv_weight, conv_bias):
    devices = lax.axis_size("space")
    channels = hidden.shape[1]
    own = channels // devices
    mine = lax.all_to_all(conv_weight, "space", split_axis=4, concat_axis=3, tiled=True)
    cells = lax.all_gather(hidden, "space", axis=0, tiled=True)
    width = cells.shape[0] // (FRAMES * ROWS)
    active = normalised(cells, norm_gain, norm_shift).reshape(FRAMES, ROWS, width, channels)
    first = active[:1]
    history = jnp.concatenate([first, first, active], axis=0)
    kernel = jnp.transpose(mine, (0, 3, 1, 2, 4)).reshape(3, channels, 9 * own)
    taps = sum(
        lax.dot_general(
            history[a : a + FRAMES].reshape(-1, channels),
            kernel[a],
            (((1,), (0,)), ((), ())),
            preferred_element_type=jnp.float32,
        )
        for a in range(3)
    ).reshape(FRAMES, ROWS, width, 3, 3, own)
    rows = phases(taps[..., 0, :, :], taps[..., 1, :, :], taps[..., 2, :, :], 1)
    cols = [phases(r[..., 0, :], r[..., 1, :], r[..., 2, :], 2) for r in rows]
    result = jnp.stack([jnp.stack(c, axis=3) for c in cols], axis=2)
    result = result.reshape(FRAMES, 2 * ROWS, 2 * width, own)
    bias = lax.dynamic_slice_in_dim(conv_bias, lax.axis_index("space") * own, own)
    decoded = (result + bias.astype(jnp.float32)).astype(jnp.bfloat16)
    return lax.all_to_all(decoded, "space", split_axis=2, concat_axis=3, tiled=True)


def fused(dims, hid_ref, gain_ref, shift_ref, w_ref, bias_ref, out_ref, acts, active, packed, weights,
          total, leaving, arrived, final, act_send, act_recv, w_send, w_recv, x_send, o_send, o_recv):
    parts, n, own, tokens, channels, width = dims
    chips = n // 2
    g, s = lax.axis_index("groups"), lax.axis_index("space")
    chip, core = s // 2, s % 2
    length = chips // 2
    z, y = chip // 2, chip % 2

    def device_at(z, y):
        return (z * 2 + y) * 2 + core

    sister = chip * 2 + 1 - core
    sends = s % parts == g

    def remote(source, target, send, recv, device, group=None):
        return pltpu.make_async_remote_copy(
            src_ref=source, dst_ref=target, send_sem=send, recv_sem=recv,
            device_id=(g if group is None else group, device), device_id_type=MESH,
        )

    barrier = pltpu.get_barrier_semaphore()
    for k in range(1, n):
        pl.semaphore_signal(barrier, inc=1, device_id=(g, lax.rem(s + k, n)), device_id_type=MESH)
    for k in range(1, parts):
        pl.semaphore_signal(barrier, inc=1, device_id=(lax.rem(g + k, parts), s), device_id_type=MESH)

    @pl.when(sends)
    def _():
        @pl.loop(0, 3)
        def _(a):
            rows = [w_ref[9 * a + i] for i in range(9)]
            for d in range(n):
                lanes = [r[:, d * own : (d + 1) * own] for r in rows]
                packed[d, 2 * a] = jnp.concatenate(lanes[:3] + lanes[6:7], axis=1)
                packed[d, 2 * a + 1] = jnp.concatenate(lanes[3:6] + lanes[7:8], axis=1)

        rows = [w_ref[9 * a + 8] for a in range(3)]
        for d in range(n):
            lanes = [r[:, d * own : (d + 1) * own] for r in rows]
            packed[d, 6] = jnp.concatenate(lanes + [jnp.zeros_like(lanes[0])], axis=1)

    acts[s] = hid_ref[...]
    pl.semaphore_wait(barrier, n - 1 + parts - 1)

    pending = []

    def go(copy):
        copy.start()
        pending.append(copy)

    guarded = []

    def go_if(wanted, copy):
        @pl.when(wanted)
        def _():
            copy.start()
        guarded.append((wanted, copy))

    chunk = tokens // PIECES
    across = device_at(z, 1 - y)

    def part(source, h):
        return acts.at[source, pl.ds(h * chunk, chunk)]

    def give(block, source, h, slot, device):
        return remote(block, part(source, h), act_send.at[slot, source, h], act_recv.at[source, h], device)

    for h in range(PIECES):
        block = hid_ref.at[pl.ds(h * chunk, chunk)]
        go_if(z < length - 1, give(block, s, h, 0, s + 4))
        go_if(z > 0, give(block, s, h, 1, s - 4))
        go(give(block, s, h, 2, across))
        go(give(block, s, h, 3, sister))

    outgoing = []
    for k in range(1, n):
        d = lax.rem(s + k, n)
        outgoing.append(remote(packed.at[d], weights.at[s], w_send.at[k], w_recv.at[s], d))

    @pl.when(sends)
    def _():
        for copy in outgoing:
            copy.start()
        weights[s] = packed[s]

    rounds = n // parts

    def relay(i):
        source = lax.rem(s // parts + rounds - i, rounds) * parts + g
        incoming = remote(weights.at[source], weights.at[source], x_send.at[i, 0], w_recv.at[source], s)
        if i == 0:
            @pl.when(s % parts != g)
            def _():
                incoming.wait_recv()
        else:
            incoming.wait_recv()
        for k in range(1, parts):
            go(remote(weights.at[source], weights.at[source], x_send.at[i, k], w_recv.at[source], s,
                      lax.rem(g + k, parts)))

    def arrival(source, h):
        give(part(source, h), source, h, 0, s).wait_recv()

    relayed = 0
    for k in range(1, length):
        for h in range(PIECES):
            for there, step, more, onward, slot in (
                (z >= k, -k, z < length - 1, s + 4, 0),
                (z + k < length, k, z > 0, s - 4, 1),
            ):
                source = lax.rem(device_at(z + step, y) + n, n)

                @pl.when(there)
                def _():
                    arrival(source, h)

                for wanted, target, line in (
                    (there & more, onward, slot), (there, across, 2), (there, sister, 3)
                ):
                    go_if(wanted, give(part(source, h), source, h, line, target))
        while relayed < rounds * k // length:
            relay(relayed)
            relayed += 1
    for k in range(length):
        source = lax.rem(z + k, length) * 4 + (1 - y) * 2 + core
        for h in range(PIECES):
            arrival(source, h)
            go(give(part(source, h), source, h, 3, sister))
    for k in range(chips):
        for h in range(PIECES):
            arrival(k * 2 + 1 - core, h)

    size = channels // GROUPS
    population = float(n * tokens * size)
    lane = lax.broadcasted_iota(jnp.int32, (8, channels), 1)

    def over_group(v):
        v = jnp.broadcast_to(jnp.sum(v, axis=0, keepdims=True), (8, channels))
        step = 1
        while step < size:
            v = v + jnp.where(lane // step % 2 == 1, pltpu.roll(v, step, 1), pltpu.roll(v, channels - step, 1))
            step *= 2
        return v[:1] / population

    def add_rows(term):
        def body(i, carry):
            v = term(acts[i].astype(jnp.float32))
            return carry + jnp.sum(v.reshape(tokens // 8, 8, channels), axis=0)
        return lax.fori_loop(0, n, body, jnp.zeros((8, channels), jnp.float32))

    average = over_group(add_rows(lambda v: v))
    spread = over_group(add_rows(lambda v: (v - average) * (v - average)))
    scale = lax.rsqrt(spread + EPSILON) * gain_ref[...]
    offset = shift_ref[...]

    @pl.loop(0, n)
    def _(i):
        v = (acts[i].astype(jnp.float32) - average) * scale + offset
        active[i] = (v / (1.0 + jnp.exp(-v))).astype(jnp.bfloat16)

    while relayed < rounds:
        relay(relayed)
        relayed += 1
    for i in range(rounds):
        for k in range(1, parts):
            source = i * parts + lax.rem(g + k, parts)
            remote(weights.at[source], weights.at[source], x_send.at[i, 0], w_recv.at[source], s).wait_recv()

    per, local = n // FRAMES, width // n
    cells = ROWS * width
    column = lax.broadcasted_iota(jnp.int32, (cells, LANES), 0) % width
    lanes = lax.broadcasted_iota(jnp.int32, (cells, LANES), 1)
    bias = bias_ref[...]

    @pl.loop(0, FRAMES)
    def _(f):
        taps = jnp.zeros((cells, 3 * LANES), jnp.float32)
        for a in range(3):
            frame = jnp.maximum(f + (a - 2), 0)
            left_side = active[pl.ds(frame * per, per)].reshape(cells, channels)
            corner = weights[:, 6].reshape(channels, LANES)
            if a < 2:
                cut = LANES - (2 - a) * own
                corner = jnp.concatenate([corner[:, cut:], corner[:, :cut]], axis=1)
            right_side = jnp.concatenate(
                [weights[:, 2 * a + b].reshape(channels, LANES) for b in range(2)] + [corner], axis=1
            )
            taps = taps + jnp.dot(left_side, right_side, preferred_element_type=jnp.float32)
        first, middle, last = (taps[:, b * LANES : (b + 1) * LANES] for b in range(3))
        last = jnp.where(
            lanes < own,
            pltpu.roll(first, own, 1),
            jnp.where(lanes < 2 * own, pltpu.roll(middle, 2 * own, 1), last),
        )
        above = jnp.concatenate([first[:width], first[:-width]], axis=0)
        below = jnp.concatenate([last[width:], last[-width:]], axis=0)
        both = []
        for r in (above + (middle + last), (first + middle) + below):
            near = pltpu.roll(r, LANES - own, 1)
            far = pltpu.roll(r, LANES - 2 * own, 1)
            back = pltpu.roll(r, own, 1)
            before = jnp.where(column == 0, r, pltpu.roll(r, 1, 0))
            after = jnp.where(column == width - 1, near, pltpu.roll(near, cells - 1, 0))
            both.append(jnp.where(lanes < own, before + near + far, back + r + after))
        joined = jnp.where(lanes < 2 * own, both[0], pltpu.roll(both[1], 2 * own, 1))
        total[pl.ds(f * cells, cells)] = joined + bias

        for d in range(n):
            for j in range(local):
                rows = total[pl.ds(f * cells + d * local + j, ROWS, stride=width), :]
                leaving[f, d, j] = rows.astype(jnp.bfloat16)
        for k in range(1, n):
            d = lax.rem(s + k, n)
            remote(leaving.at[f, d], arrived.at[f, s], o_send.at[f, k], o_recv.at[f, s], d).start()
        arrived[f, s] = leaving[f, s]

    quarter = lax.broadcasted_iota(jnp.int32, (ROWS, LANES), 1) // own

    @pl.loop(0, FRAMES)
    def _(f):
        for k in range(1, n):
            source = lax.rem(s + n - k, n)
            remote(arrived.at[f, source], arrived.at[f, source], o_send.at[f, k], o_recv.at[f, source], s).wait()
        for q in range(n // 4):
            for j in range(local):
                pieces = [arrived[f, 4 * q + i, j].astype(jnp.float32) for i in range(4)]
                for phase in range(4):
                    whole = pieces[phase]
                    for i in range(4):
                        turned = pieces[i] if i == phase else pltpu.roll(pieces[i], (i - phase) % 4 * own, 1)
                        whole = turned if i == 0 else jnp.where(quarter == i, turned, whole)
                    pr, pc = phase // 2, phase % 2
                    at = f * (ROWS * 4 * local) + (pr * local + j) * 2 + pc
                    final[q, pl.ds(at, ROWS, stride=4 * local), :] = whole

    for q in range(n // 4):
        out_ref[:, q * LANES : (q + 1) * LANES] = final[q].astype(jnp.bfloat16)

    for copy in pending:
        copy.wait_send()

    for wanted, copy in guarded:
        @pl.when(wanted)
        def _():
            copy.wait_send()

    @pl.when(sends)
    def _():
        for copy in outgoing:
            copy.wait_send()


def fused_shards(hidden, norm_gain, norm_shift, conv_weight, conv_bias):
    n, parts = lax.axis_size("space"), lax.axis_size("groups")
    tokens, channels = hidden.shape
    own = channels // n
    width = n * tokens // (FRAMES * ROWS)
    local = width // n
    bias = lax.dynamic_slice_in_dim(conv_bias, lax.axis_index("space") * own, own)
    bias = jnp.tile(bias.astype(jnp.float32), 4)[None]
    rows = FRAMES * 2 * ROWS * 2 * local
    bf16, f32 = jnp.bfloat16, jnp.float32
    dma = pltpu.SemaphoreType.DMA
    rounds = n // parts
    out = pl.pallas_call(
        functools.partial(fused, (parts, n, own, tokens, channels, width)),
        out_shape=jax.ShapeDtypeStruct((rows, channels), bf16),
        in_specs=[pl.BlockSpec(memory_space=pltpu.VMEM)] * 5,
        out_specs=pl.BlockSpec(memory_space=pltpu.VMEM),
        scratch_shapes=[
            pltpu.VMEM((n, tokens, channels), bf16),
            pltpu.VMEM((n, tokens, channels), bf16),
            pltpu.VMEM((n, 7, own, LANES), bf16),
            pltpu.VMEM((n, 7, own, LANES), bf16),
            pltpu.VMEM((n * tokens, LANES), f32),
            pltpu.VMEM((FRAMES, n, local, ROWS, LANES), bf16),
            pltpu.VMEM((FRAMES, n, local, ROWS, LANES), bf16),
            pltpu.VMEM((n // 4, rows, LANES), f32),
            dma((4, n, PIECES)),
            dma((n, PIECES)),
            dma((n,)),
            dma((n,)),
            dma((rounds, parts)),
            dma((FRAMES, n)),
            dma((FRAMES, n)),
        ],
        compiler_params=pltpu.CompilerParams(
            collective_id=0, has_side_effects=True, vmem_limit_bytes=60 * 1024 * 1024
        ),
    )(
        hidden,
        norm_gain[None],
        norm_shift[None],
        conv_weight.reshape(27, own, channels),
        bias,
    )
    return out.reshape(FRAMES, 2 * ROWS, 2 * local, channels)


def pick(hidden, norm_gain, norm_shift, conv_weight, conv_bias):
    n, parts = lax.axis_size("space"), lax.axis_size("groups")
    own = hidden.shape[1] // n
    suits = own * 4 == LANES and n % 4 == 0 and n % parts == 0 and hidden.shape[0] % 16 == 0
    body = fused_shards if suits else shards
    return body(hidden, norm_gain, norm_shift, conv_weight, conv_bias)


def solution(mesh):
    placed = (P(("groups", "space"), None), P(), P(), P(None, None, None, "space", None), P())
    return jax.shard_map(
        pick,
        mesh=mesh,
        in_specs=placed,
        out_specs=P("groups", None, "space", None),
        check_vma=False,
    )
```

```python
import functools

import jax
import jax.numpy as jnp
from jax import lax
from jax.experimental import pallas as pl
from jax.experimental.pallas import tpu as pltpu
from jax.sharding import PartitionSpec as P

GROUPS = 32
FRAMES = 4
ROWS = 16
EPSILON = 1e-06
LANES = 128
PIECES = 2
MESH = pl.DeviceIdType.MESH


def normalised(hidden, gain, shift):
    cells, channels = hidden.shape
    values = hidden.astype(jnp.float32)
    member = (
        jnp.arange(channels)[:, None] // (channels // GROUPS)
        == jnp.arange(channels)[None, :] // (channels // GROUPS)
    ).astype(jnp.float32)
    population = float(cells * (channels // GROUPS))

    def spread_out(v):
        return jnp.dot(v[None], member, precision=lax.Precision.HIGHEST)[0] / population

    average = spread_out(jnp.sum(values, axis=0))
    spread = spread_out(jnp.sum((values - average) ** 2, axis=0))
    scale = lax.rsqrt(spread + EPSILON) * gain
    return jax.nn.silu((values - average) * scale + shift).astype(jnp.bfloat16)


def clamp_shift(x, axis, step):
    length = x.shape[axis]
    if step < 0:
        return jnp.concatenate(
            [lax.slice_in_dim(x, 0, 1, axis=axis), lax.slice_in_dim(x, 0, length - 1, axis=axis)],
            axis=axis,
        )
    return jnp.concatenate(
        [lax.slice_in_dim(x, 1, length, axis=axis), lax.slice_in_dim(x, length - 1, length, axis=axis)],
        axis=axis,
    )


def phases(first, middle, last, axis):
    early = clamp_shift(first, axis, -1) + (middle + last)
    late = (first + middle) + clamp_shift(last, axis, 1)
    return early, late


def shards(hidden, norm_gain, norm_shift, conv_weight, conv_bias):
    devices = lax.axis_size("space")
    channels = hidden.shape[1]
    own = channels // devices
    mine = lax.all_to_all(conv_weight, "space", split_axis=4, concat_axis=3, tiled=True)
    cells = lax.all_gather(hidden, "space", axis=0, tiled=True)
    width = cells.shape[0] // (FRAMES * ROWS)
    active = normalised(cells, norm_gain, norm_shift).reshape(FRAMES, ROWS, width, channels)
    first = active[:1]
    history = jnp.concatenate([first, first, active], axis=0)
    kernel = jnp.transpose(mine, (0, 3, 1, 2, 4)).reshape(3, channels, 9 * own)
    taps = sum(
        lax.dot_general(
            history[a : a + FRAMES].reshape(-1, channels),
            kernel[a],
            (((1,), (0,)), ((), ())),
            preferred_element_type=jnp.float32,
        )
        for a in range(3)
    ).reshape(FRAMES, ROWS, width, 3, 3, own)
    rows = phases(taps[..., 0, :, :], taps[..., 1, :, :], taps[..., 2, :, :], 1)
    cols = [phases(r[..., 0, :], r[..., 1, :], r[..., 2, :], 2) for r in rows]
    result = jnp.stack([jnp.stack(c, axis=3) for c in cols], axis=2)
    result = result.reshape(FRAMES, 2 * ROWS, 2 * width, own)
    bias = lax.dynamic_slice_in_dim(conv_bias, lax.axis_index("space") * own, own)
    decoded = (result + bias.astype(jnp.float32)).astype(jnp.bfloat16)
    return lax.all_to_all(decoded, "space", split_axis=2, concat_axis=3, tiled=True)


def fused(dims, hid_ref, gain_ref, shift_ref, w_ref, bias_ref, out_ref, acts, active, packed, weights,
          total, leaving, arrived, final, act_send, act_recv, w_send, w_recv, x_send, o_send, o_recv):
    parts, n, own, tokens, channels, width = dims
    chips = n // 2
    g, s = lax.axis_index("groups"), lax.axis_index("space")
    chip, core = s // 2, s % 2
    length = chips // 2
    z, y = chip // 2, chip % 2

    def device_at(z, y):
        return (z * 2 + y) * 2 + core

    sister = chip * 2 + 1 - core
    sends = s % parts == g

    def remote(source, target, send, recv, device, group=None):
        return pltpu.make_async_remote_copy(
            src_ref=source, dst_ref=target, send_sem=send, recv_sem=recv,
            device_id=(g if group is None else group, device), device_id_type=MESH,
        )

    barrier = pltpu.get_barrier_semaphore()
    for k in range(1, n):
        pl.semaphore_signal(barrier, inc=1, device_id=(g, lax.rem(s + k, n)), device_id_type=MESH)
    for k in range(1, parts):
        pl.semaphore_signal(barrier, inc=1, device_id=(lax.rem(g + k, parts), s), device_id_type=MESH)

    acts[s] = hid_ref[...]
    pl.semaphore_wait(barrier, n - 1 + parts - 1)

    pending = []

    def go(copy):
        copy.start()
        pending.append(copy)

    guarded = []

    def go_if(wanted, copy):
        @pl.when(wanted)
        def _():
            copy.start()
        guarded.append((wanted, copy))

    chunk = tokens // PIECES
    across = device_at(z, 1 - y)

    def part(source, h):
        return acts.at[source, pl.ds(h * chunk, chunk)]

    def give(block, source, h, slot, device):
        return remote(block, part(source, h), act_send.at[slot, source, h], act_recv.at[source, h], device)

    for h in range(PIECES):
        block = hid_ref.at[pl.ds(h * chunk, chunk)]
        go_if(z < length - 1, give(block, s, h, 0, s + 4))
        go_if(z > 0, give(block, s, h, 1, s - 4))
        go(give(block, s, h, 2, across))
        go(give(block, s, h, 3, sister))

    @pl.when(sends)
    def _():
        @pl.loop(0, 3)
        def _(a):
            rows = [w_ref[9 * a + i] for i in range(9)]
            for d in range(n):
                lanes = [r[:, d * own : (d + 1) * own] for r in rows]
                packed[d, 2 * a] = jnp.concatenate(lanes[:3] + lanes[6:7], axis=1)
                packed[d, 2 * a + 1] = jnp.concatenate(lanes[3:6] + lanes[7:8], axis=1)

        rows = [w_ref[9 * a + 8] for a in range(3)]
        for d in range(n):
            lanes = [r[:, d * own : (d + 1) * own] for r in rows]
            packed[d, 6] = jnp.concatenate(lanes + [jnp.zeros_like(lanes[0])], axis=1)

    outgoing = []
    for k in range(1, n):
        d = lax.rem(s + k, n)
        outgoing.append(remote(packed.at[d], weights.at[s], w_send.at[k], w_recv.at[s], d))

    @pl.when(sends)
    def _():
        for copy in outgoing:
            copy.start()
        weights[s] = packed[s]

    rounds = n // parts

    def relay(i):
        source = lax.rem(s // parts + rounds - i, rounds) * parts + g
        incoming = remote(weights.at[source], weights.at[source], x_send.at[i, 0], w_recv.at[source], s)
        if i == 0:
            @pl.when(s % parts != g)
            def _():
                incoming.wait_recv()
        else:
            incoming.wait_recv()
        for k in range(1, parts):
            go(remote(weights.at[source], weights.at[source], x_send.at[i, k], w_recv.at[source], s,
                      lax.rem(g + k, parts)))

    def arrival(source, h):
        give(part(source, h), source, h, 0, s).wait_recv()

    relayed = 0
    for k in range(1, length):
        for h in range(PIECES):
            for there, step, more, onward, slot in (
                (z >= k, -k, z < length - 1, s + 4, 0),
                (z + k < length, k, z > 0, s - 4, 1),
            ):
                source = lax.rem(device_at(z + step, y) + n, n)

                @pl.when(there)
                def _():
                    arrival(source, h)

                for wanted, target, line in (
                    (there & more, onward, slot), (there, across, 2), (there, sister, 3)
                ):
                    go_if(wanted, give(part(source, h), source, h, line, target))
        while relayed < min(rounds, rounds * (k + 1) // length):
            relay(relayed)
            relayed += 1
    for k in range(length):
        source = lax.rem(z + k, length) * 4 + (1 - y) * 2 + core
        for h in range(PIECES):
            arrival(source, h)
            go(give(part(source, h), source, h, 3, sister))
    for k in range(chips):
        for h in range(PIECES):
            arrival(k * 2 + 1 - core, h)

    size = channels // GROUPS
    population = float(n * tokens * size)
    lane = lax.broadcasted_iota(jnp.int32, (8, channels), 1)

    def over_group(v):
        v = jnp.broadcast_to(jnp.sum(v, axis=0, keepdims=True), (8, channels))
        step = 1
        while step < size:
            v = v + jnp.where(lane // step % 2 == 1, pltpu.roll(v, step, 1), pltpu.roll(v, channels - step, 1))
            step *= 2
        return v[:1] / population

    def add_rows(term):
        def body(i, carry):
            v = term(acts[i].astype(jnp.float32))
            return carry + jnp.sum(v.reshape(tokens // 8, 8, channels), axis=0)
        return lax.fori_loop(0, n, body, jnp.zeros((8, channels), jnp.float32))

    average = over_group(add_rows(lambda v: v))
    spread = over_group(add_rows(lambda v: (v - average) * (v - average)))
    scale = lax.rsqrt(spread + EPSILON) * gain_ref[...]
    offset = shift_ref[...]

    @pl.loop(0, n)
    def _(i):
        v = (acts[i].astype(jnp.float32) - average) * scale + offset
        active[i] = (v / (1.0 + jnp.exp(-v))).astype(jnp.bfloat16)

    while relayed < rounds:
        relay(relayed)
        relayed += 1
    for i in range(rounds):
        for k in range(1, parts):
            source = i * parts + lax.rem(g + k, parts)
            remote(weights.at[source], weights.at[source], x_send.at[i, 0], w_recv.at[source], s).wait_recv()

    per, local = n // FRAMES, width // n
    cells = ROWS * width
    column = lax.broadcasted_iota(jnp.int32, (cells, LANES), 0) % width
    lanes = lax.broadcasted_iota(jnp.int32, (cells, LANES), 1)
    turn = lax.broadcasted_iota(jnp.int32, (8, LANES), 1) // own
    row = jnp.broadcast_to(bias_ref[...].astype(jnp.float32), (8, channels))
    held = row[:, :LANES]
    for q in range(1, n // 4):
        held = jnp.where(s // 4 == q, row[:, q * LANES : (q + 1) * LANES], held)
    wide = held
    for i in range(4):
        copies = held
        for j in range(4):
            copies = jnp.where(turn == j, held if i == j else pltpu.roll(held, (j - i) % 4 * own, 1), copies)
        wide = jnp.where(s % 4 == i, copies, wide)
    bias = wide[:1]

    @pl.loop(0, FRAMES)
    def _(f):
        taps = jnp.zeros((cells, 3 * LANES), jnp.float32)
        for a in range(3):
            frame = jnp.maximum(f + (a - 2), 0)
            left_side = active[pl.ds(frame * per, per)].reshape(cells, channels)
            corner = weights[:, 6].reshape(channels, LANES)
            if a < 2:
                cut = LANES - (2 - a) * own
                corner = jnp.concatenate([corner[:, cut:], corner[:, :cut]], axis=1)
            right_side = jnp.concatenate(
                [weights[:, 2 * a + b].reshape(channels, LANES) for b in range(2)] + [corner], axis=1
            )
            taps = taps + jnp.dot(left_side, right_side, preferred_element_type=jnp.float32)
        first, middle, last = (taps[:, b * LANES : (b + 1) * LANES] for b in range(3))
        last = jnp.where(
            lanes < own,
            pltpu.roll(first, own, 1),
            jnp.where(lanes < 2 * own, pltpu.roll(middle, 2 * own, 1), last),
        )
        above = jnp.concatenate([first[:width], first[:-width]], axis=0)
        below = jnp.concatenate([last[width:], last[-width:]], axis=0)
        both = []
        for r in (above + (middle + last), (first + middle) + below):
            near = pltpu.roll(r, LANES - own, 1)
            far = pltpu.roll(r, LANES - 2 * own, 1)
            back = pltpu.roll(r, own, 1)
            before = jnp.where(column == 0, r, pltpu.roll(r, 1, 0))
            after = jnp.where(column == width - 1, near, pltpu.roll(near, cells - 1, 0))
            both.append(jnp.where(lanes < own, before + near + far, back + r + after))
        joined = jnp.where(lanes < 2 * own, both[0], pltpu.roll(both[1], 2 * own, 1))
        total[pl.ds(f * cells, cells)] = joined + bias

        for d in range(n):
            for j in range(local):
                rows = total[pl.ds(f * cells + d * local + j, ROWS, stride=width), :]
                leaving[f, d, j] = rows.astype(jnp.bfloat16)
        for k in range(1, n):
            d = lax.rem(s + k, n)
            remote(leaving.at[f, d], arrived.at[f, s], o_send.at[f, k], o_recv.at[f, s], d).start()
        arrived[f, s] = leaving[f, s]

    quarter = lax.broadcasted_iota(jnp.int32, (ROWS, LANES), 1) // own

    @pl.loop(0, FRAMES)
    def _(f):
        for k in range(1, n):
            source = lax.rem(s + n - k, n)
            remote(arrived.at[f, source], arrived.at[f, source], o_send.at[f, k], o_recv.at[f, source], s).wait()
        for q in range(n // 4):
            for j in range(local):
                pieces = [arrived[f, 4 * q + i, j].astype(jnp.float32) for i in range(4)]
                for phase in range(4):
                    whole = pieces[phase]
                    for i in range(4):
                        turned = pieces[i] if i == phase else pltpu.roll(pieces[i], (i - phase) % 4 * own, 1)
                        whole = turned if i == 0 else jnp.where(quarter == i, turned, whole)
                    pr, pc = phase // 2, phase % 2
                    at = f * (ROWS * 4 * local) + (pr * local + j) * 2 + pc
                    final[q, pl.ds(at, ROWS, stride=4 * local), :] = whole

    for q in range(n // 4):
        out_ref[:, q * LANES : (q + 1) * LANES] = final[q].astype(jnp.bfloat16)

    for copy in pending:
        copy.wait_send()

    for wanted, copy in guarded:
        @pl.when(wanted)
        def _():
            copy.wait_send()

    @pl.when(sends)
    def _():
        for copy in outgoing:
            copy.wait_send()


def fused_shards(hidden, norm_gain, norm_shift, conv_weight, conv_bias):
    n, parts = lax.axis_size("space"), lax.axis_size("groups")
    tokens, channels = hidden.shape
    own = channels // n
    width = n * tokens // (FRAMES * ROWS)
    local = width // n
    rows = FRAMES * 2 * ROWS * 2 * local
    bf16, f32 = jnp.bfloat16, jnp.float32
    dma = pltpu.SemaphoreType.DMA
    rounds = n // parts
    out = pl.pallas_call(
        functools.partial(fused, (parts, n, own, tokens, channels, width)),
        out_shape=jax.ShapeDtypeStruct((rows, channels), bf16),
        in_specs=[pl.BlockSpec(memory_space=pltpu.VMEM)] * 5,
        out_specs=pl.BlockSpec(memory_space=pltpu.VMEM),
        scratch_shapes=[
            pltpu.VMEM((n, tokens, channels), bf16),
            pltpu.VMEM((n, tokens, channels), bf16),
            pltpu.VMEM((n, 7, own, LANES), bf16),
            pltpu.VMEM((n, 7, own, LANES), bf16),
            pltpu.VMEM((n * tokens, LANES), f32),
            pltpu.VMEM((FRAMES, n, local, ROWS, LANES), bf16),
            pltpu.VMEM((FRAMES, n, local, ROWS, LANES), bf16),
            pltpu.VMEM((n // 4, rows, LANES), f32),
            dma((4, n, PIECES)),
            dma((n, PIECES)),
            dma((n,)),
            dma((n,)),
            dma((rounds, parts)),
            dma((FRAMES, n)),
            dma((FRAMES, n)),
        ],
        compiler_params=pltpu.CompilerParams(
            collective_id=0, has_side_effects=True, vmem_limit_bytes=60 * 1024 * 1024
        ),
    )(
        hidden,
        norm_gain[None],
        norm_shift[None],
        conv_weight.reshape(27, own, channels),
        conv_bias[None],
    )
    return out.reshape(FRAMES, 2 * ROWS, 2 * local, channels)


def pick(hidden, norm_gain, norm_shift, conv_weight, conv_bias):
    n, parts = lax.axis_size("space"), lax.axis_size("groups")
    own = hidden.shape[1] // n
    suits = own * 4 == LANES and n % 4 == 0 and n % parts == 0 and hidden.shape[0] % 16 == 0
    body = fused_shards if suits else shards
    return body(hidden, norm_gain, norm_shift, conv_weight, conv_bias)


def solution(mesh):
    placed = (P(("groups", "space"), None), P(), P(), P(None, None, None, "space", None), P())
    return jax.shard_map(
        pick,
        mesh=mesh,
        in_specs=placed,
        out_specs=P("groups", None, "space", None),
        check_vma=False,
    )
```
